32 devices in a mesh: clu: 16 (over z, y, x), col: 2 (over core).
Axes of the slice: x: 2, y: 2, z: 4, core: 2. Of those that a mesh axis runs over, the one named last changes fastest.
Arguments:
- features: bfloat16 [16384, 2048], P('clu', 'col'), may hold values from -6 to 6
- adj_mask: int32 [16384, 1024], P('clu'), may hold values 0 or 1
- degrees: int32 [16384], P('clu'), may hold values from 12 to 39
- halo_rows: int32 [16, 16, 32], P('clu'), may hold values from 0 to 1023
- halo_dest: int32 [16, 16, 32], P('clu'), may hold values from 0 to 1023
- halo_count: int32 [16, 16], P('clu'), may hold values from 0 to 32, as said below
- w_first: bfloat16 [2048, 2048], P(None, 'col'), may hold values from -0.75 to 0.75
- b_first: bfloat16 [2048], P('col'), may hold values from -3 to 3
- w_second: bfloat16 [2048, 2048], P(None, 'col'), may hold values from -0.75 to 0.75
- b_second: bfloat16 [2048], P('col'), may hold values from -3 to 3
- out_grad: bfloat16 [16384, 2048], P('clu', 'col'), may hold values from -6 to 6
Outputs:
- first_out: bfloat16 [16384, 2048], P('clu', 'col')
- second_out: bfloat16 [16384, 2048], P('clu', 'col')
- input_grad: float32 [16384, 2048], P('clu', 'col')
- wgrad_first: float32 [2048, 2048], P(None, 'col')
- bgrad_first: float32 [2048], P('col')
- wgrad_second: float32 [2048, 2048], P(None, 'col')
- bgrad_second: float32 [2048], P('col')
The draws below stay inside these ranges and needn't reach their ends.
Inputs may be any that keep to these rules, and one draw needn't show every extreme that they name: `halo_count`: entry [c, p] counts the used slots, the first ones, from cluster p to cluster c; a cluster sends nothing to itself; every cluster receives 32 from some other cluster.
All inputs are finite; a program needn't handle non-finite values. No bound on the sum of `adj_mask` on one device may be relied on, other than what follows from the above.
Results may differ from the reference program's by a relative error of at most 0.011.
Values may be sent and summed in bfloat16 or wider, within the bound.
A program may use at most 192 MiB of HBM per device.

```python
import jax
import jax.numpy as jnp
from jax import lax

F = 2048
NODES = 1024
CAP = 32
CLUSTERS = 16
NODES_ALL = 16384


def draw_halo_count(key, part):
    counts = jax.random.randint(key, (CLUSTERS, CLUSTERS), 3 * CAP // 8, CAP + 1)
    receiver = jnp.arange(CLUSTERS, dtype=jnp.int32)[:, None]
    sender = jnp.arange(CLUSTERS, dtype=jnp.int32)[None, :]
    offset = jax.random.randint(jax.random.fold_in(key, 7), (), 1, CLUSTERS)
    counts = jnp.where(sender == (receiver + offset) % CLUSTERS, CAP, counts)
    counts = jnp.where(sender == receiver, 0, counts)
    return counts.astype(jnp.int32)


def plant(values, stream_key, smallest, top_value):
    longest = values.shape.index(max(values.shape))
    spots = []
    for shift in (0, 1):
        where = [jax.random.randint(jax.random.fold_in(stream_key, axis), (), 0, length) for axis, length in enumerate(values.shape)]
        where[longest] = (where[longest] + shift) % values.shape[longest]
        spots.append(tuple(where))
    return values.at[spots[0]].set(smallest).at[spots[1]].set(top_value)


def shard_levels(key, shape, shards, least, largest):
    gain = 1.0
    for position, shards_of in shards:
        heights = jax.random.uniform(jax.random.fold_in(jax.random.fold_in(key, 6), position), (shards_of,), jnp.float32, least / len(shards), largest / len(shards))
        gain = gain * jnp.repeat(jnp.exp(heights), shape[position] // shards_of).reshape((-1,) + (1,) * (len(shape) - 1 - position))
    return gain


def noise(key, shape, scale, reach, cuts=(), kind=jnp.bfloat16):
    result = scale * jax.random.normal(key, shape, jnp.float32)
    if cuts:
        result = result * shard_levels(key, shape, cuts, -0.22, 0.18)
    return jnp.clip(result, -reach, reach).astype(kind)


def setup_inputs(seed: int = 0) -> dict:
    seeds = jax.random.split(jax.random.key(seed), 12)
    features = noise(seeds[0], (NODES_ALL, F), 1.0, 6.0, ((0, 16), (1, 2)))
    adj_mask = plant((jax.random.randint(seeds[1], (NODES_ALL, NODES), 0, max(2, NODES // 16)) < 1).astype(jnp.int32), jax.random.fold_in(seeds[1], 1), 0, 1)
    degrees = plant(jax.random.randint(seeds[2], (NODES_ALL,), 12, 40), jax.random.fold_in(seeds[2], 1), 12, 39).astype(jnp.int32)
    halo_rows = plant(jax.random.randint(seeds[3], (CLUSTERS, CLUSTERS, CAP), 0, NODES), jax.random.fold_in(seeds[3], 1), 0, NODES - 1).astype(jnp.int32)
    halo_dest = plant(jax.random.randint(seeds[4], (CLUSTERS, CLUSTERS, CAP), 0, NODES), jax.random.fold_in(seeds[4], 1), 0, NODES - 1).astype(jnp.int32)
    halo_count = draw_halo_count(jax.random.fold_in(seeds[11], 71), 0)
    w_first = noise(seeds[6], (F, F), (F // 32) ** -0.5, 0.75, ((1, 2),))
    b_first = noise(seeds[7], (F,), 0.5, 3.0, ((0, 2),))
    w_second = noise(seeds[8], (F, F), (F // 32) ** -0.5, 0.75, ((1, 2),))
    b_second = noise(seeds[9], (F,), 0.5, 3.0, ((0, 2),))
    out_grad = noise(seeds[10], (NODES_ALL, F), 1.0, 6.0, ((0, 16), (1, 2)))
    return dict(features=features, adj_mask=adj_mask, degrees=degrees, halo_rows=halo_rows, halo_dest=halo_dest, halo_count=halo_count, w_first=w_first, b_first=b_first, w_second=w_second, b_second=b_second, out_grad=out_grad)


@jax.custom_vjp
def low(v):
    return lax.optimization_barrier(v.astype(jnp.bfloat16)).astype(jnp.float32)

@jax.custom_vjp
def low_back(v):
    return v

def low_keep(v):
    return (low(v), None)

def low_pass(kept, grad):
    return (grad,)

def back_keep(v):
    return (v, None)

def back_low(kept, grad):
    return (low(grad),)
low.defvjp(low_keep, low_pass)
low_back.defvjp(back_keep, back_low)

def reference(features, adj_mask, degrees, halo_rows, halo_dest, halo_count, w_first, b_first, w_second, b_second, out_grad):
    highest = lax.Precision.HIGHEST
    scale = (1.0 / (degrees.astype(jnp.float32) + 1.0))[:, None]
    adjacency = adj_mask.astype(jnp.float32).reshape(CLUSTERS, NODES, NODES)
    senders = jnp.arange(CLUSTERS, dtype=jnp.int32)[:, None, None] * NODES
    flat_rows = (senders + halo_rows).astype(jnp.int32)
    flat_rows = jnp.transpose(flat_rows, (1, 0, 2)).reshape(CLUSTERS, CLUSTERS * CAP).astype(jnp.int32)
    targets = halo_dest.reshape(CLUSTERS, CLUSTERS * CAP).astype(jnp.int32)
    slot_ids = jnp.arange(CAP, dtype=jnp.int32)[None, None, :]
    live = (slot_ids < halo_count[:, :, None]).reshape(CLUSTERS, CLUSTERS * CAP)
    node_ids = jnp.arange(NODES, dtype=jnp.int32)[:, None]

    def layer(values, weight, bias):

        def cluster(pieces):
            adj_block, rows_block, dest_block, live_block, own_rows = pieces
            halo = low_back(values[rows_block])
            incidence = ((dest_block[None, :] == node_ids) & live_block[None, :]).astype(jnp.float32)
            inner = jnp.dot(adj_block, own_rows, precision=highest)
            inner = inner + jnp.dot(incidence, halo, precision=highest)
            return inner + 2.0 * own_rows
        inner = lax.map(jax.checkpoint(cluster), (adjacency, flat_rows, targets, live, values.reshape(CLUSTERS, NODES, F)))
        inner = inner.reshape(NODES_ALL, F)
        mixed = low(scale * low_back(inner))
        pre_act = low_back(jnp.dot(mixed, weight, precision=highest) + bias)
        return jax.nn.gelu(pre_act, approximate=True)

    def forward(values, weight_one, bias_one, weight_two, bias_two):
        first = low_back(low(layer(values, weight_one, bias_one)))
        second = low(layer(first, weight_two, bias_two))
        return (first, second)
    primals = (features.astype(jnp.float32), w_first.astype(jnp.float32), b_first.astype(jnp.float32), w_second.astype(jnp.float32), b_second.astype(jnp.float32))
    outputs, pull = jax.vjp(forward, *primals)
    first, second = outputs
    grads = pull((jnp.zeros_like(first), out_grad.astype(jnp.float32)))
    return (first.astype(jnp.bfloat16), second.astype(jnp.bfloat16), grads[0], grads[1], grads[2], grads[3], grads[4])
```

```python
import jax
import jax.numpy as jnp
from jax import lax
from jax.sharding import PartitionSpec as P

F32 = jnp.float32
BF16 = jnp.bfloat16


def activate(pre_act):
    return jax.nn.gelu(pre_act, approximate=True)


def dot(a, b, dims):
    return lax.dot_general(a, b, (dims, ((), ())), preferred_element_type=F32)


ROWS_COLS = ((1,), (0,))
TRANSPOSED = ((0,), (0,))
BY_ROWS = ((1,), (1,))


def flip(x, bit, members):
    return lax.ppermute(x, "clu", [(i, i ^ (1 << bit)) for i in range(members)])


def total_rows(part, order, members):
    index = lax.axis_index("clu")
    for bit in order:
        half = part.shape[0] // 2
        mine = (index >> bit) & 1
        keep = lax.dynamic_slice_in_dim(part, mine * half, half, 0)
        give = lax.dynamic_slice_in_dim(part, (1 - mine) * half, half, 0)
        got = flip(give, bit, members)
        part = (keep.astype(F32) + got.astype(F32)).astype(BF16)
    for bit in reversed(order):
        mine = (index >> bit) & 1
        got = flip(part, bit, members)
        part = jnp.where(
            mine == 0, jnp.concatenate([part, got]), jnp.concatenate([got, part])
        )
    return part


def total_small(x, bits, members):
    for bit in range(bits):
        x = x + flip(x, bit, members)
    return x


def shards(
    features,
    adj_mask,
    degrees,
    halo_rows,
    halo_dest,
    halo_count,
    w_first,
    b_first,
    w_second,
    b_second,
    out_grad,
):
    nodes, width = features.shape
    peers = halo_rows.shape[1]
    slots = halo_rows.shape[2]
    bits = peers.bit_length() - 1
    col = lax.axis_index("col")
    scale = (1.0 / (degrees.astype(F32) + 1.0))[:, None]
    node_ids = jnp.arange(nodes)
    adjacency = (adj_mask + 2 * (node_ids[:, None] == node_ids[None, :])).astype(BF16)
    live = (jnp.arange(slots)[None, :] < halo_count[0][:, None]).reshape(-1)
    targets = halo_dest[0].reshape(-1)
    incidence = ((targets[None, :] == node_ids[:, None]) & live[None, :]).astype(BF16)
    sources = halo_rows[0].reshape(-1)
    pick = (sources[:, None] == node_ids[None, :]).astype(BF16)

    def swap(x):
        return lax.ppermute(x, "col", [(0, 1), (1, 0)])

    def exchange(rows):
        out = lax.all_to_all(
            rows.reshape(peers, slots, width), "clu", split_axis=0, concat_axis=0, tiled=True
        )
        return out.reshape(peers * slots, width)

    def halves(weight):
        own = lax.dynamic_slice_in_dim(weight, col * width, width, 0)
        other = lax.dynamic_slice_in_dim(weight, (1 - col) * width, width, 0)
        return own, other

    def forward(values, weights, bias):
        incoming = exchange(dot(pick, values, ROWS_COLS).astype(BF16))
        inner = dot(adjacency, values, ROWS_COLS) + dot(incidence, incoming, ROWS_COLS)
        mixed = (scale * inner).astype(BF16)
        other = swap(mixed)
        pre_act = dot(mixed, weights[0], ROWS_COLS) + dot(other, weights[1], ROWS_COLS)
        return (mixed, other), pre_act + bias.astype(F32)

    def weight_sum(mixed, grad_pre):
        terms = [dot(m, grad_pre, TRANSPOSED).astype(BF16) for m in mixed]
        cut = nodes_cut(terms[0].shape[0])
        orders = bit_orders(bits)
        own = jnp.concatenate(
            [
                total_rows(terms[0][:cut], orders[0], peers),
                total_rows(terms[0][cut:], orders[2], peers),
            ]
        )
        other = jnp.concatenate(
            [
                total_rows(terms[1][:cut], orders[1], peers),
                total_rows(terms[1][cut:], orders[3], peers),
            ]
        )
        first = jnp.where(col == 0, own, other)
        second = jnp.where(col == 0, other, own)
        return jnp.concatenate([first, second]).astype(F32)

    def backward(grad_out, mixed, pre_act, weights):
        unused, pull_act = jax.vjp(activate, pre_act)
        grad_pre = pull_act(grad_out.astype(F32))[0].astype(BF16)
        grad_weight = weight_sum(mixed, grad_pre)
        grad_bias = total_small(jnp.sum(grad_pre.astype(F32), axis=0), bits, peers)
        sent = swap(dot(grad_pre, weights[1], BY_ROWS).astype(BF16))
        grad_mixed = dot(grad_pre, weights[0], BY_ROWS) + sent.astype(F32)
        scaled = (scale * grad_mixed).astype(BF16)
        returned = exchange(dot(incidence, scaled, TRANSPOSED).astype(BF16))
        grad_in = dot(adjacency, scaled, TRANSPOSED) + dot(pick, returned, TRANSPOSED)
        return grad_in, grad_weight, grad_bias

    weights_one = halves(w_first)
    weights_two = halves(w_second)
    mixed_one, pre_one = forward(features, weights_one, b_first)
    first_out = activate(pre_one).astype(BF16)
    mixed_two, pre_two = forward(first_out, weights_two, b_second)
    second_out = activate(pre_two).astype(BF16)
    grad_first, wgrad_second, bgrad_second = backward(out_grad, mixed_two, pre_two, weights_two)
    input_grad, wgrad_first, bgrad_first = backward(
        grad_first.astype(BF16), mixed_one, pre_one, weights_one
    )
    return (first_out, second_out, input_grad, wgrad_first, bgrad_first, wgrad_second, bgrad_second)


def nodes_cut(rows):
    return rows * 3 // 4


def bit_orders(bits):
    up = list(range(bits))
    x_first = up
    y_first = up[1::-1] + up[2:]
    z_first = up[2:] + up[:2]
    z_then_y = up[2:] + up[1::-1]
    return x_first, y_first, z_first, z_then_y


def solution(mesh):
    return jax.shard_map(
        shards,
        mesh=mesh,
        in_specs=(
            P("clu", "col"),
            P("clu", None),
            P("clu"),
            P("clu", None, None),
            P("clu", None, None),
            P("clu", None),
            P(None, "col"),
            P("col"),
            P(None, "col"),
            P("col"),
            P("clu", "col"),
        ),
        out_specs=(
            P("clu", "col"),
            P("clu", "col"),
            P("clu", "col"),
            P(None, "col"),
            P("col"),
            P(None, "col"),
            P("col"),
        ),
        check_vma=False,
    )
```
